32 devices in a mesh: row: 2 (over y), theta: 4 (over x, core), gz: 4 (over z).
Axes of the slice: x: 2, y: 2, z: 4, core: 2. Of those that a mesh axis runs over, the one named last changes fastest.
Arguments:
- state_start: float32 [6, 8, 128, 1024], P(None, 'row', 'gz', 'theta'), may hold values from -1.2 to 1.2
- state_section: float32 [6, 8, 128, 1024], P(None, 'row', 'gz', 'theta'), may hold values from -1.5 to 4, as said below
- phase: int32 [8, 128, 1024], P('row', 'gz', 'theta'), may hold values 0 or 1
- cutoff: int32 [4], replicated, may hold values from 1 to 63
Outputs:
- state_next: float32 [6, 8, 128, 1024], P(None, 'row', 'gz', 'theta')
The draws below stay inside these ranges and needn't reach their ends.
Inputs may be any that keep to these rules, and one draw needn't show every extreme that they name: `state_section`: channel 0 (density) lies in 0.5 to 2.0, channels 1 to 3 (momenta) in -1.5 to 1.5, channel 4 (total energy) in 2.5 to 4.0, channel 5 (jet mass density) in 0 to 1.0.
All inputs are finite; a program needn't handle non-finite values. No bound on the sum of `phase` on one device may be relied on, other than what follows from the above.
Results may differ from the reference program's by a relative error of at most 0.0003.
Values sent between devices are 32-bit elements; how exact they have to be, the bound alone decides.
A program may use at most 64 MiB of HBM per device.

```python
import math
import jax
import jax.numpy as jnp
from jax import lax

NT = 1024
NF = 4
KMODES = 64
NR = 8
NZ = 128


def draw_state_section(key, part):
    subkeys = jax.random.split(jax.random.fold_in(key, 11), 4)
    grid_shape = (NR, NZ, NT)
    density = jax.random.uniform(subkeys[0], grid_shape, minval=0.5, maxval=2.0)
    momenta = jnp.clip(0.3 * jax.random.normal(subkeys[1], (3, NR, NZ, NT)), -1.5, 1.5)
    energy = jax.random.uniform(subkeys[2], grid_shape, minval=2.5, maxval=4.0)
    jet_mass = jax.random.uniform(subkeys[3], grid_shape, minval=0.0, maxval=1.0)
    return jnp.concatenate([density[None], momenta, energy[None], jet_mass[None]], 0).astype(jnp.float32)


def place_ends(values, key, least, largest):
    longest = values.shape.index(max(values.shape))
    spots = []
    for shift in (0, 1):
        where = [jax.random.randint(jax.random.fold_in(key, axis), (), 0, length) for axis, length in enumerate(values.shape)]
        where[longest] = (where[longest] + shift) % values.shape[longest]
        spots.append(tuple(where))
    return values.at[spots[0]].set(least).at[spots[1]].set(largest)


def block_scale(own_key, dims, cuts, low, high):
    def one(position, parts):
        draws = jax.random.uniform(jax.random.fold_in(jax.random.fold_in(own_key, 6), position), (parts,), jnp.float32, low / len(cuts), high / len(cuts))
        return jnp.repeat(jnp.exp(draws), dims[position] // parts).reshape((-1,) + (1,) * (len(dims) - position - 1))

    gain = one(*cuts[0])
    for cut in cuts[1:]:
        gain = gain * one(*cut)
    return gain


def gaussian(rng, dims, scale, most, pieces=(), kind=jnp.bfloat16):
    gain = block_scale(rng, dims, pieces, -0.22, 0.18) if pieces else 1.0
    result = jax.random.normal(rng, dims, jnp.float32) * scale * gain
    return jnp.minimum(jnp.maximum(result, -most), most).astype(kind)


def setup_inputs(seed: int = 0) -> dict:
    splits = jax.random.split(jax.random.key(seed), 5)
    return {
        "state_start": gaussian(splits[0], (6, NR, NZ, NT), 0.2, 1.2, ((1, 2), (2, 4), (3, 4)), jnp.float32),
        "state_section": draw_state_section(jax.random.fold_in(splits[4], 71), 0),
        "phase": place_ends((jax.random.randint(splits[2], (NR, NZ, NT), 0, 3) < 1).astype(jnp.int32), jax.random.fold_in(splits[2], 1), 0, 1),
        "cutoff": place_ends(jax.random.randint(splits[3], (NF,), 1, KMODES), jax.random.fold_in(splits[3], 1), 1, KMODES - 1).astype(jnp.int32),
    }


split_speed = 10.0
time_step = 0.05
weno_epsilon = 1e-6
liquid_ratio = 4.4
gas_ratio = 1.4
liquid_stiffness = 0.6


def pressure_of(state, phase):
    density = state[0]
    kinetic = 0.5 * (state[1] * state[1] + state[2] * state[2] + state[3] * state[3]) / density
    liquid = phase == 1
    heat_ratio = jnp.where(liquid, liquid_ratio, gas_ratio)
    stiffness = jnp.where(liquid, liquid_stiffness, 0.0)
    return (heat_ratio - 1.0) * (state[4] - kinetic) - heat_ratio * stiffness


def weno_face(far_left, near_left, centre, near_right, far_right):
    smooth_left = 13.0 / 12.0 * (far_left - 2.0 * near_left + centre) ** 2 + 0.25 * (far_left - 4.0 * near_left + 3.0 * centre) ** 2
    smooth_mid = 13.0 / 12.0 * (near_left - 2.0 * centre + near_right) ** 2 + 0.25 * (near_left - near_right) ** 2
    smooth_right = 13.0 / 12.0 * (centre - 2.0 * near_right + far_right) ** 2 + 0.25 * (3.0 * centre - 4.0 * near_right + far_right) ** 2
    weight_left = 0.1 / (weno_epsilon + smooth_left) ** 2
    weight_mid = 0.6 / (weno_epsilon + smooth_mid) ** 2
    weight_right = 0.3 / (weno_epsilon + smooth_right) ** 2
    weight_sum = weight_left + weight_mid + weight_right
    value_left = (2.0 * far_left - 7.0 * near_left + 11.0 * centre) / 6.0
    value_mid = (-near_left + 5.0 * centre + 2.0 * near_right) / 6.0
    value_right = (2.0 * centre + 5.0 * near_right - far_right) / 6.0
    return (weight_left * value_left + weight_mid * value_mid + weight_right * value_right) / weight_sum


def face_fluxes(padded_line, array_axis, component):
    density = padded_line[0]
    velocity = padded_line[component] / density
    pressure_field = padded_line[6]
    conserved = padded_line[:6]
    flux_rows = [conserved[channel] * velocity for channel in range(6)]
    flux_rows[component] = flux_rows[component] + pressure_field
    flux_rows[4] = flux_rows[4] + pressure_field * velocity
    physical = jnp.stack(flux_rows)
    upward = 0.5 * (physical + split_speed * conserved)
    downward = 0.5 * (physical - split_speed * conserved)
    face_count = padded_line.shape[array_axis] - 5

    def shifted(values, offset):
        return lax.slice_in_dim(values, offset, offset + face_count, axis=array_axis)

    upwind_part = weno_face(shifted(upward, 0), shifted(upward, 1), shifted(upward, 2), shifted(upward, 3), shifted(upward, 4))
    downwind_part = weno_face(shifted(downward, 5), shifted(downward, 4), shifted(downward, 3), shifted(downward, 2), shifted(downward, 1))
    return upwind_part + downwind_part


def tendency(centre_cells, radial_line, axial_line, azimuth_line, cycle_start):
    cycle_count = centre_cells.shape[1]
    radial_flux = face_fluxes(radial_line, 1, 1)
    axial_flux = face_fluxes(axial_line, 2, 3)
    azimuth_flux = face_fluxes(azimuth_line, 3, 2)
    cycle_index = (cycle_start + lax.iota(jnp.int32, cycle_count + 1)).astype(centre_cells.dtype)
    face_radius = cycle_index[None, :, None, None]
    cell_radius = face_radius[:, :-1] + 0.5
    weighted = face_radius * radial_flux
    div_radial = (weighted[:, 1:] - weighted[:, :-1]) / cell_radius
    div_axial = axial_flux[:, :, 1:] - axial_flux[:, :, :-1]
    angle_step = 2.0 * math.pi / NT
    div_azimuth = (azimuth_flux[..., 1:] - azimuth_flux[..., :-1]) / (cell_radius * angle_step)
    density = centre_cells[0]
    swirl_speed = centre_cells[2] / density
    radius = cell_radius[0]
    source_radial = (centre_cells[2] * swirl_speed + centre_cells[6]) / radius
    source_swirl = -centre_cells[1] * swirl_speed / radius
    zero_field = jnp.zeros_like(density)
    source = jnp.stack([zero_field, source_radial, source_swirl, zero_field, zero_field, zero_field])
    return source - div_radial - div_axial - div_azimuth


def across_axis(partner):
    sign_flip = jnp.array([1.0, -1.0, -1.0, 1.0, 1.0, 1.0, 1.0], partner.dtype)[:, None, None, None]
    return partner[:, ::-1] * sign_flip


def reference(state_start, state_section, phase, cutoff):
    pressure_field = pressure_of(state_section, phase)
    fields = jnp.concatenate([state_section, pressure_field[None]], 0)
    total_depth = fields.shape[2]
    block_size = math.gcd(total_depth, 8)
    block_count = total_depth // block_size

    def one_block(number):
        positions = (number * block_size - 3 + lax.iota(jnp.int32, block_size + 6)) % total_depth
        axial_line = jnp.take(fields, positions.astype(jnp.int32), axis=2)
        centre_cells = axial_line[:, :, 3:-3]
        partner = jnp.roll(centre_cells[:, 0:3], -(NT // 2), axis=3)
        outer_rim = jnp.repeat(centre_cells[:, -1:], 3, axis=1)
        radial_line = jnp.concatenate([across_axis(partner), centre_cells, outer_rim], 1)
        azimuth_line = jnp.concatenate([centre_cells[..., -3:], centre_cells, centre_cells[..., :3]], 3)
        tendencies = tendency(centre_cells, radial_line, axial_line, azimuth_line, 0)
        start_index = (number * block_size).astype(jnp.int32)
        start_block = lax.dynamic_slice_in_dim(state_start, start_index, block_size, 2)
        section_block = lax.dynamic_slice_in_dim(state_section, start_index, block_size, 2)
        return 0.75 * start_block + 0.25 * (section_block + time_step * tendencies)

    block_results = lax.map(one_block, lax.iota(jnp.int32, block_count))
    advanced = jnp.moveaxis(block_results, 0, 2).reshape(state_start.shape)
    inner_block = advanced[:, :NF]
    spectrum = jnp.fft.rfft(inner_block, axis=3)
    mode_index = lax.iota(jnp.int32, NT // 2 + 1)
    kept_modes = mode_index[None, :] <= cutoff[:, None]
    filtered = jnp.fft.irfft(spectrum * kept_modes[None, :, None, :], n=NT, axis=3).astype(advanced.dtype)
    return jnp.concatenate([filtered, advanced[:, NF:]], 1)
```

```python
import functools
import math

import jax
import jax.numpy as jnp
from jax import lax
from jax.experimental import pallas as pl
from jax.experimental.pallas import tpu as pltpu
from jax.sharding import PartitionSpec as P

KMODES = 64
HALO = 3
LANES = 128
SUB = 8

split_speed = 10.0
time_step = 0.05
weno_epsilon = 1e-06
liquid_ratio = 4.4
gas_ratio = 1.4
liquid_stiffness = 0.6


def pressure_of(state, phase):
    kinetic = 0.5 * (state[1] * state[1] + state[2] * state[2] + state[3] * state[3]) / state[0]
    liquid = phase == 1
    heat_ratio = jnp.where(liquid, liquid_ratio, gas_ratio)
    stiffness = jnp.where(liquid, liquid_stiffness, 0.0)
    return (heat_ratio - 1.0) * (state[4] - kinetic) - heat_ratio * stiffness


def upwind_terms(f, count):
    D = [f[i + 1] - f[i] for i in range(count + 4)]
    G = [0.75 * D[i] for i in range(count + 4)]
    s = [D[i + 1] - D[i] for i in range(count + 3)]
    e = [s[i] - s[i + 1] for i in range(count + 2)]
    q = [s[i] * s[i] + 3.0 * weno_epsilon for i in range(count + 3)]
    out = []
    for m in range(count + 1):
        b0 = q[m] + G[m + 1] * (D[m + 1] + s[m])
        b1 = q[m + 1] + G[m + 1] * D[m + 2]
        b2 = q[m + 2] + G[m + 2] * (D[m + 2] - s[m + 2])
        B0 = b0 * (3.0 * b0)
        B1 = b1 * b1
        B2 = b2 * b2
        B2d = B2 + B2
        numer = B1 * (B2d * e[m] + B0 * e[m + 1])
        denom = B1 * (B2 + B0) + B0 * B2d
        r = pl.reciprocal(denom, approx=True)
        r = r * (2.0 - denom * r)
        out.append(numer * r)
    return out


def line_faces(q, velocity, pressure, component, channel, count):
    cells = count + 6
    flux = []
    for i in range(cells):
        if channel == 4:
            value = (q[i] + pressure(i)) * velocity[i]
        else:
            value = q[i] * velocity[i]
            if channel == component:
                value = value + pressure(i)
        flux.append(value)
    scaled = [split_speed * q[i] for i in range(cells)]
    plus = [flux[i] + scaled[i] for i in range(cells)]
    minus = [flux[i] - scaled[i] for i in range(cells)]
    up = upwind_terms(plus, count)
    down = upwind_terms(minus[::-1], count)[::-1]
    faces = []
    for m in range(count + 1):
        linear = 7.0 * (flux[m + 2] + flux[m + 3]) - (flux[m + 1] + flux[m + 4])
        linear = linear + ((scaled[m + 4] - scaled[m + 1]) - 3.0 * (scaled[m + 3] - scaled[m + 2]))
        faces.append(linear + (up[m] + down[m]))
    return faces


def prepare_kernel(sec, phase, press, bottom, top, zlo, zhi, ft, tlo, thi):
    R, Z, T = press.shape
    for r in range(R):
        press[r] = pressure_of([sec[c, r] for c in range(6)], phase[r])
    for c in range(7):
        def row(r):
            return sec[c, r] if c < 6 else press[r]
        for g in range(HALO):
            bottom[c, g] = row(g)
            top[c, g] = row(R - HALO + g)
        for r in range(R):
            value = row(r)
            zlo[c, r] = value[:HALO]
            zhi[c, r] = value[Z - HALO :]
        per = LANES // Z
        for n in range(R // per):
            block = jnp.concatenate([row(n * per + i) for i in range(per)], 0)
            turned = jnp.transpose(block)
            ft[c, :, n * LANES : (n + 1) * LANES] = turned
            tlo[c, :, n * LANES : (n + 1) * LANES] = turned[:HALO]
            thi[c, :, n * LANES : (n + 1) * LANES] = turned[T - HALO :]


def plane_kernel(angle_step, radius, start, sec, press, zlo, zhi, ft, tlo, thi, out, fz, fe, tt, zt):
    _, R, Z, T = sec.shape
    NL = R * Z
    nl = T // LANES
    for c in range(7):
        for n in range(NL // LANES):
            lanes = slice(n * LANES, (n + 1) * LANES)
            fe[c, n, SUB : SUB + T] = ft[c, :, lanes]
            fe[c, n, SUB - HALO : SUB] = tlo[c, :, lanes]
            fe[c, n, SUB + T : SUB + T + HALO] = thi[c, :, lanes]
        for r in range(R):
            for n in range(nl):
                lanes = slice(n * LANES, (n + 1) * LANES)
                fz[c, r, n, SUB : SUB + Z] = sec[c, r, :, lanes] if c < 6 else press[r, :, lanes]
                fz[c, r, n, SUB - HALO : SUB] = zlo[c, r, :, lanes]
                fz[c, r, n, SUB + Z : SUB + Z + HALO] = zhi[c, r, :, lanes]
    tstride = T // SUB
    chunk = 8
    for lane in range(NL // LANES):

        def theta_chunk(k, carry):
            base = k * chunk

            def at(c, i):
                return fe[c, lane, pl.ds(base + (i + SUB - HALO), SUB, stride=tstride), :]

            velocity = [at(2, i) / at(0, i) for i in range(chunk + 6)]
            for c in range(6):
                q = [at(c, i) for i in range(chunk + 6)]
                faces = line_faces(q, velocity, lambda i: at(6, i), 2, c, chunk)
                for m in range(chunk):
                    tt[c, lane, pl.ds(base + m, SUB, stride=tstride), :] = faces[m + 1] - faces[m]
            return carry

        lax.fori_loop(0, tstride // chunk, theta_chunk, 0)
    zstride = Z // SUB

    def axial(step, carry):
        r = step // nl
        n = step - r * nl

        def at(c, i):
            return fz[c, r, n, pl.ds(i + SUB - HALO, SUB, stride=zstride), :]

        velocity = [at(3, i) / at(0, i) for i in range(zstride + 6)]
        for c in range(6):
            q = [at(c, i) for i in range(zstride + 6)]
            faces = line_faces(q, velocity, lambda i: at(6, i), 3, c, zstride)
            for m in range(zstride):
                zt[c, r, n, pl.ds(m, SUB, stride=zstride), :] = faces[m + 1] - faces[m]
        return carry

    lax.fori_loop(0, R * nl, axial, 0)
    per = LANES // Z
    for c in range(6):
        for n in range(NL // LANES):
            turned = jnp.transpose(tt[c, n])
            for i in range(per):
                r = n * per + i
                cell_radius = radius[r] + 0.5
                axial_part = jnp.concatenate([zt[c, r, m] for m in range(nl)], 1)
                tend = -(1.0 / 12.0) * axial_part - turned[i * Z : (i + 1) * Z] * (
                    1.0 / (12.0 * angle_step * cell_radius)
                )
                if c == 1:
                    tend = tend + (sec[2, r] * sec[2, r] / sec[0, r] + press[r]) / cell_radius
                if c == 2:
                    tend = tend - sec[1, r] * sec[2, r] / (sec[0, r] * cell_radius)
                out[c, r] = 0.75 * start[c, r] + 0.25 * (sec[c, r] + time_step * tend)


def radial_kernel(nf, radius, place, part, sec, press, mirror, lower, upper, table, out, coef, lo, hi):
    _, R, Z, T = sec.shape
    first = place[0] == 1
    last = place[1] == 1
    for c in range(7):
        sign = -1.0 if c in (1, 2) else 1.0
        for g in range(HALO):
            rim = sec[c, R - 1] if c < 6 else press[R - 1]
            lo[c, g] = jnp.where(first, sign * mirror[c, HALO - 1 - g], lower[c, g])
            hi[c, g] = jnp.where(last, rim, upper[c, g])

    def radial(n, carry):
        zs = n // (T // LANES)
        rows = pl.ds(pl.multiple_of(zs * SUB, SUB), SUB)
        lanes = pl.ds(pl.multiple_of((n - zs * (T // LANES)) * LANES, LANES), LANES)

        def at(c, i):
            if i < HALO:
                return lo[c, i, rows, lanes]
            if i >= R + HALO:
                return hi[c, i - R - HALO, rows, lanes]
            return sec[c, i - HALO, rows, lanes] if c < 6 else press[i - HALO, rows, lanes]

        velocity = [at(1, i) / at(0, i) for i in range(R + 6)]
        for c in range(6):
            q = [at(c, i) for i in range(R + 6)]
            faces = line_faces(q, velocity, lambda i: at(6, i), 1, c, R)
            weighted = [radius[i] * faces[i] for i in range(R + 1)]
            for i in range(R):
                scale = 0.25 * time_step / (12.0 * (radius[i] + 0.5))
                out[c, i, rows, lanes] = (
                    part[c, i, rows, lanes] - (weighted[i + 1] - weighted[i]) * scale
                )
        return carry

    lax.fori_loop(0, (Z // SUB) * (T // LANES), radial, 0)
    for c in range(6):
        block = jnp.concatenate([out[c, r] for r in range(nf)], 0)
        coef[c] = jnp.dot(
            block, table[...], preferred_element_type=jnp.float32, precision=lax.Precision.HIGHEST
        )


def inverse_kernel(nf, place, adv, coef, weights, table, out):
    _, R, Z, T = adv.shape
    first = place[0] == 1

    @pl.when(first)
    def _():
        for c in range(6):
            rows = [coef[c, r * Z : (r + 1) * Z] * weights[r : r + 1] for r in range(nf)]
            value = lax.dot_general(
                jnp.concatenate(rows, 0),
                table[...],
                (((1,), (1,)), ((), ())),
                preferred_element_type=jnp.float32,
                precision=lax.Precision.HIGHEST,
            )
            for r in range(nf):
                out[c, r] = value[r * Z : (r + 1) * Z]
            for r in range(nf, R):
                out[c, r] = adv[c, r]

    @pl.when(jnp.logical_not(first))
    def _():
        out[...] = adv[...]


def build_table(positions, mode_count, length):
    orders = lax.iota(jnp.int32, mode_count)
    phases = positions[:, None] * orders[None, :] % length
    angles = phases.astype(jnp.float32) * (2.0 * math.pi / length)
    return jnp.concatenate([jnp.cos(angles), jnp.sin(angles)], 1)


def cycle_weights(cutoff, mode_count, length):
    orders = lax.iota(jnp.int32, mode_count)
    mode_scale = jnp.where(orders == 0, 1.0 / length, 2.0 / length)
    kept_modes = orders[None, :] <= cutoff[:, None]
    weight_half = jnp.where(kept_modes, mode_scale[None, :], 0.0)
    return jnp.concatenate([weight_half, weight_half], 1)


def shape_of(*dims):
    return jax.ShapeDtypeStruct(dims, jnp.float32)


def summed(coef, theta_count, theta_id):
    half = coef.shape[1] // 2
    odd = theta_id % 2 == 1
    swap = [(i, i ^ 1) for i in range(theta_count)]
    low, high = coef[:, :half], coef[:, half:]
    keep = jnp.where(odd, high, low) + lax.ppermute(jnp.where(odd, low, high), "theta", swap)
    distance = 2
    while distance < theta_count:
        keep = keep + lax.ppermute(keep, "theta", [(i, i ^ distance) for i in range(theta_count)])
        distance *= 2
    other = lax.ppermute(keep, "theta", swap)
    return jnp.concatenate([jnp.where(odd, other, keep), jnp.where(odd, keep, other)], 1)


def shards(state_start, state_section, phase, cutoff):
    row_count = lax.axis_size("row")
    row_id = lax.axis_index("row")
    theta_count = lax.axis_size("theta")
    theta_id = lax.axis_index("theta")
    gz_count = lax.axis_size("gz")
    _, R, Z, T = state_section.shape
    NL = R * Z
    nf = cutoff.shape[0]
    length = T * theta_count
    whole = pl.BlockSpec(memory_space=pltpu.VMEM)
    scalar = pl.BlockSpec(memory_space=pltpu.SMEM)
    limit = pltpu.CompilerParams(vmem_limit_bytes=48 * 1024 * 1024)

    press, bottom, top, zlo, zhi, ft, tlo, thi = pl.pallas_call(
        prepare_kernel,
        out_shape=[
            shape_of(R, Z, T),
            shape_of(7, HALO, Z, T),
            shape_of(7, HALO, Z, T),
            shape_of(7, R, HALO, T),
            shape_of(7, R, HALO, T),
            shape_of(7, T, NL),
            shape_of(7, HALO, NL),
            shape_of(7, HALO, NL),
        ],
        in_specs=[whole] * 2,
        out_specs=[whole] * 8,
        compiler_params=limit,
        name="prepare",
    )(state_section, phase)

    def along(value, axis, count, step):
        return lax.ppermute(value, axis, [(i, (i + step) % count) for i in range(count)])

    near_tlo = along(thi, "theta", theta_count, 1)
    near_thi = along(tlo, "theta", theta_count, -1)
    near_zlo = along(zhi, "gz", gz_count, 1)
    near_zhi = along(zlo, "gz", gz_count, -1)
    mirror = lax.ppermute(
        bottom, ("row", "theta"), [(i, (i + theta_count // 2) % theta_count) for i in range(theta_count)]
    )
    lower = lax.ppermute(top, "row", [(i, i + 1) for i in range(row_count - 1)])
    upper = lax.ppermute(bottom, "row", [(i + 1, i) for i in range(row_count - 1)])

    radius = (row_id * R + lax.iota(jnp.int32, R + 1)).astype(jnp.float32)
    place = jnp.stack([row_id == 0, row_id == row_count - 1]).astype(jnp.int32)
    part = pl.pallas_call(
        functools.partial(plane_kernel, 2.0 * math.pi / length),
        out_shape=shape_of(6, R, Z, T),
        in_specs=[scalar] + [whole] * 8,
        out_specs=whole,
        scratch_shapes=[
            pltpu.VMEM((7, R, T // LANES, Z + 2 * SUB, LANES), jnp.float32),
            pltpu.VMEM((7, NL // LANES, T + 2 * SUB, LANES), jnp.float32),
            pltpu.VMEM((6, NL // LANES, T, LANES), jnp.float32),
            pltpu.VMEM((6, R, T // LANES, Z, LANES), jnp.float32),
        ],
        compiler_params=limit,
        cost_estimate=pl.CostEstimate(flops=60_000_000, bytes_accessed=8_000_000, transcendentals=0),
        name="plane",
    )(radius, state_start, state_section, press, near_zlo, near_zhi, ft, near_tlo, near_thi)

    positions = theta_id * T + lax.iota(jnp.int32, T)
    table = build_table(positions, KMODES, length)
    weights = cycle_weights(cutoff, KMODES, length)
    advanced, coef = pl.pallas_call(
        functools.partial(radial_kernel, nf),
        out_shape=[shape_of(6, R, Z, T), shape_of(6, nf * Z, 2 * KMODES)],
        in_specs=[scalar] * 2 + [whole] * 7,
        out_specs=[whole] * 2,
        scratch_shapes=[
            pltpu.VMEM((7, HALO, Z, T), jnp.float32),
            pltpu.VMEM((7, HALO, Z, T), jnp.float32),
        ],
        compiler_params=limit,
        name="radial",
    )(radius, place, part, state_section, press, mirror, lower, upper, table)

    coef = summed(coef, theta_count, theta_id)
    return pl.pallas_call(
        functools.partial(inverse_kernel, nf),
        out_shape=shape_of(6, R, Z, T),
        in_specs=[scalar] + [whole] * 4,
        out_specs=whole,
        compiler_params=limit,
        name="inverse",
    )(place, advanced, coef, weights, table)


def solution(mesh):
    in_specs = (
        P(None, "row", "gz", "theta"),
        P(None, "row", "gz", "theta"),
        P("row", "gz", "theta"),
        P(),
    )
    out_specs = P(None, "row", "gz", "theta")
    return jax.shard_map(shards, mesh=mesh, in_specs=in_specs, out_specs=out_specs, check_vma=False)
```

```python
import functools
import math

import jax
import jax.numpy as jnp
from jax import lax
from jax.experimental import pallas as pl
from jax.experimental.pallas import tpu as pltpu
from jax.sharding import PartitionSpec as P

KMODES = 64
HALO = 3
LANES = 128
SUB = 8

split_speed = 10.0
time_step = 0.05
weno_epsilon = 1e-06
liquid_ratio = 4.4
gas_ratio = 1.4
liquid_stiffness = 0.6


def pressure_of(state, phase):
    kinetic = 0.5 * (state[1] * state[1] + state[2] * state[2] + state[3] * state[3]) / state[0]
    liquid = phase == 1
    heat_ratio = jnp.where(liquid, liquid_ratio, gas_ratio)
    stiffness = jnp.where(liquid, liquid_stiffness, 0.0)
    return (heat_ratio - 1.0) * (state[4] - kinetic) - heat_ratio * stiffness


def upwind_terms(f, count):
    D = [f[i + 1] - f[i] for i in range(count + 4)]
    G = [0.75 * D[i] for i in range(count + 4)]
    s = [D[i + 1] - D[i] for i in range(count + 3)]
    e = [s[i] - s[i + 1] for i in range(count + 2)]
    q = [s[i] * s[i] + 3.0 * weno_epsilon for i in range(count + 3)]
    out = []
    for m in range(count + 1):
        b0 = q[m] + G[m + 1] * (D[m + 1] + s[m])
        b1 = q[m + 1] + G[m + 1] * D[m + 2]
        b2 = q[m + 2] + G[m + 2] * (D[m + 2] - s[m + 2])
        B0 = b0 * (3.0 * b0)
        B1 = b1 * b1
        B2 = b2 * b2
        B2d = B2 + B2
        numer = B1 * (B2d * e[m] + B0 * e[m + 1])
        denom = B1 * (B2 + B0) + B0 * B2d
        r = pl.reciprocal(denom, approx=True)
        r = r * (2.0 - denom * r)
        out.append(numer * r)
    return out


def line_faces(q, velocity, pressure, component, channel, count):
    cells = count + 6
    flux = []
    for i in range(cells):
        if channel == 4:
            value = (q[i] + pressure(i)) * velocity[i]
        else:
            value = q[i] * velocity[i]
            if channel == component:
                value = value + pressure(i)
        flux.append(value)
    scaled = [split_speed * q[i] for i in range(cells)]
    plus = [flux[i] + scaled[i] for i in range(cells)]
    minus = [flux[i] - scaled[i] for i in range(cells)]
    up = upwind_terms(plus, count)
    down = upwind_terms(minus[::-1], count)[::-1]
    faces = []
    for m in range(count + 1):
        linear = 7.0 * (flux[m + 2] + flux[m + 3]) - (flux[m + 1] + flux[m + 4])
        linear = linear + ((scaled[m + 4] - scaled[m + 1]) - 3.0 * (scaled[m + 3] - scaled[m + 2]))
        faces.append(linear + (up[m] + down[m]))
    return faces


def fused_kernel(
    nf, angle_step, counts, radius, start, sec, phase, table, out, coef,
    press, fz, zph, fe, tt, zt, lo, loph, hi, hiph, own, got, half, cross, whole_sum,
    lo_send, lo_recv, hi_send, hi_recv, z_send, z_recv, t_send, t_recv, c_send, c_recv,
):
    row_count, theta_count, gz_count = counts
    _, R, Z, T = sec.shape
    NL = R * Z
    nl = T // LANES
    per = LANES // Z
    chunks = Z // SUB
    row = lax.axis_index("row")
    theta = lax.axis_index("theta")
    gz = lax.axis_index("gz")
    first = row == 0
    last = row == row_count - 1
    MESH = pl.DeviceIdType.MESH

    right = lax.rem(theta + 1, theta_count)
    left = lax.rem(theta + theta_count - 1, theta_count)
    across = lax.rem(theta + theta_count // 2, theta_count)
    ahead = lax.rem(gz + 1, gz_count)
    behind = lax.rem(gz + gz_count - 1, gz_count)
    odd = lax.rem(theta, 2)
    pair = theta + 1 - 2 * odd

    barrier = pltpu.get_barrier_semaphore()

    def greet(**axes):
        pl.semaphore_signal(barrier, inc=1, device_id=axes, device_id_type=MESH)

    for t in (right, left, across):
        greet(theta=t)
    greet(gz=ahead)
    greet(gz=behind)

    @pl.when(jnp.logical_not(first))
    def _():
        greet(row=row - 1)

    @pl.when(jnp.logical_not(last))
    def _():
        greet(row=row + 1)

    @pl.when(jnp.logical_or(first, last))
    def _():
        pl.semaphore_wait(barrier, 6)

    if row_count > 2:

        @pl.when(jnp.logical_not(jnp.logical_or(first, last)))
        def _():
            pl.semaphore_wait(barrier, 7)

    def remote(src, dst, send, recv, axes):
        return pltpu.make_async_remote_copy(
            src_ref=src, dst_ref=dst, send_sem=send, recv_sem=recv, device_id=axes, device_id_type=MESH
        )

    def slab(k, g0, to, toph, send, recv, axes):
        zs = pl.ds(k * SUB, SUB)
        return (
            remote(sec.at[:, pl.ds(g0, HALO), zs], to.at[:, :, zs], send.at[k, 0], recv.at[k, 0], axes),
            remote(phase.at[pl.ds(g0, HALO), zs], toph.at[:, zs], send.at[k, 1], recv.at[k, 1], axes),
        )

    def mirrored(k):
        return slab(k, 0, lo, loph, lo_send, lo_recv, dict(theta=across))

    def upward(k):
        return slab(k, R - HALO, lo, loph, lo_send, lo_recv, dict(row=row + 1))

    def downward(k):
        return slab(k, 0, hi, hiph, hi_send, hi_recv, dict(row=row - 1))

    def start_all(copies):
        for copy in copies:
            copy.start()

    def mirror_start(k):
        @pl.when(first)
        def _():
            start_all(mirrored(k))

    mirror_start(0)

    def upward_from(k):
        zs = pl.ds(k * SUB, SUB)
        g0 = R - HALO
        axes = dict(row=row + 1)
        return (
            remote(sec.at[:, pl.ds(g0, HALO), zs], lo.at[:, :, zs], c_send.at[k, 3], lo_recv.at[k, 0], axes),
            remote(phase.at[pl.ds(g0, HALO), zs], loph.at[:, zs], c_send.at[k, 4], lo_recv.at[k, 1], axes),
        )

    for k in range(chunks):

        @pl.when(jnp.logical_not(last))
        def _():
            start_all(upward_from(k))

        @pl.when(jnp.logical_not(first))
        def _():
            start_all(downward(k))

    def axial_copies():
        out = []
        for n in range(nl):
            lanes = pl.ds(n * LANES, LANES)
            for side, (src0, dst0, axes) in enumerate(
                ((Z - SUB, 0, dict(gz=ahead)), (0, SUB + Z, dict(gz=behind)))
            ):
                rows = pl.ds(src0, SUB)
                out.append(
                    remote(
                        sec.at[:, :, rows, lanes],
                        fz.at[pl.ds(0, 6), :, n, pl.ds(dst0, SUB)],
                        z_send.at[n, side, 0],
                        z_recv.at[n, side, 0],
                        axes,
                    )
                )
                out.append(
                    remote(
                        phase.at[:, rows, lanes],
                        zph.at[:, n, side],
                        z_send.at[n, side, 1],
                        z_recv.at[n, side, 1],
                        axes,
                    )
                )
        return out

    start_all(axial_copies())

    for r in range(R):
        press[r] = pressure_of([sec[c, r] for c in range(6)], phase[r])

    def field(c, r):
        return sec[c, r] if c < 6 else press[r]

    for c in range(7):
        for n in range(NL // LANES):
            block = jnp.concatenate([field(c, n * per + i) for i in range(per)], 0)
            fe[c, n, SUB : SUB + T] = jnp.transpose(block)
    for c in range(7):
        for r in range(R):
            value = field(c, r)
            for n in range(nl):
                fz[c, r, n, SUB : SUB + Z] = value[:, n * LANES : (n + 1) * LANES]

    def theta_copies():
        return (
            remote(
                fe.at[:, :, pl.ds(T, SUB)], fe.at[:, :, pl.ds(0, SUB)], t_send.at[0], t_recv.at[0], dict(theta=right)
            ),
            remote(
                fe.at[:, :, pl.ds(SUB, SUB)],
                fe.at[:, :, pl.ds(SUB + T, SUB)],
                t_send.at[1],
                t_recv.at[1],
                dict(theta=left),
            ),
        )

    start_all(theta_copies())
    for k in range(1, chunks):
        mirror_start(k)

    tstride = T // SUB
    chunk = SUB
    pieces = tstride // chunk

    def theta_piece(lane, k):
        base = k * chunk

        def at(c, i):
            return fe[c, lane, pl.ds(base + (i + SUB - HALO), SUB, stride=tstride), :]

        velocity = [at(2, i) / at(0, i) for i in range(chunk + 6)]
        for c in range(6):
            q = [at(c, i) for i in range(chunk + 6)]
            faces = line_faces(q, velocity, lambda i: at(6, i), 2, c, chunk)
            for m in range(chunk):
                tt[c, lane, pl.ds(base + m, SUB, stride=tstride), :] = faces[m + 1] - faces[m]

    for lane in range(NL // LANES):

        @pl.loop(1, pieces - 1)
        def _(k):
            theta_piece(lane, k)

    for copy in theta_copies():
        copy.wait()
    for lane in range(NL // LANES):

        @pl.loop(0, 2)
        def _(k):
            theta_piece(lane, k * (pieces - 1))

    for copy in axial_copies():
        copy.wait()
    for side, row0 in enumerate((0, SUB + Z)):
        for r in range(R):
            for n in range(nl):
                cells = [fz[c, r, n, row0 : row0 + SUB] for c in range(6)]
                fz[6, r, n, row0 : row0 + SUB] = pressure_of(cells, zph[r, n, side])
    zstride = Z // SUB

    @pl.loop(0, R * nl)
    def _(step):
        r = step // nl
        n = step - r * nl

        def at(c, i):
            return fz[c, r, n, pl.ds(i + SUB - HALO, SUB, stride=zstride), :]

        velocity = [at(3, i) / at(0, i) for i in range(zstride + 6)]
        for c in range(6):
            q = [at(c, i) for i in range(zstride + 6)]
            faces = line_faces(q, velocity, lambda i: at(6, i), 3, c, zstride)
            for m in range(zstride):
                zt[c, r, n, pl.ds(m, SUB, stride=zstride), :] = faces[m + 1] - faces[m]

    for c in range(6):
        for n in range(NL // LANES):
            turned = jnp.transpose(tt[c, n])
            for i in range(per):
                r = n * per + i
                cell_radius = radius[r] + 0.5
                axial_part = jnp.concatenate([zt[c, r, m] for m in range(nl)], 1)
                tend = -(1.0 / 12.0) * axial_part - turned[i * Z : (i + 1) * Z] * (
                    1.0 / (12.0 * angle_step * cell_radius)
                )
                if c == 1:
                    tend = tend + (sec[2, r] * sec[2, r] / sec[0, r] + press[r]) / cell_radius
                if c == 2:
                    tend = tend - sec[1, r] * sec[2, r] / (sec[0, r] * cell_radius)
                out[c, r] = 0.75 * start[c, r] + 0.25 * (sec[c, r] + time_step * tend)

    @pl.when(last)
    def _():
        for g in range(HALO):
            for c in range(6):
                hi[c, g] = sec[c, R - 1]
            hiph[g] = phase[R - 1]

    sign = jnp.where(first, -1.0, 1.0).astype(jnp.float32)

    def radial_chunk(k):
        rows = pl.ds(k * SUB, SUB)

        @pl.loop(0, nl)
        def _(n):
            lanes = pl.ds(pl.multiple_of(n * LANES, LANES), LANES)
            ghosts = {}
            for i in range(HALO):
                g = jnp.where(first, HALO - 1 - i, i)
                cells = [lo[c, g, rows, lanes] for c in range(6)]
                cells = [sign * v if c in (1, 2) else v for c, v in enumerate(cells)]
                ghosts[i] = cells + [pressure_of(cells, loph[g, rows, lanes])]
                cells = [hi[c, i, rows, lanes] for c in range(6)]
                ghosts[R + HALO + i] = cells + [pressure_of(cells, hiph[i, rows, lanes])]

            def at(c, i):
                if i in ghosts:
                    return ghosts[i][c]
                return sec[c, i - HALO, rows, lanes] if c < 6 else press[i - HALO, rows, lanes]

            velocity = [at(1, i) / at(0, i) for i in range(R + 6)]
            for c in range(6):
                q = [at(c, i) for i in range(R + 6)]
                faces = line_faces(q, velocity, lambda i: at(6, i), 1, c, R)
                weighted = [radius[i] * faces[i] for i in range(R + 1)]
                for i in range(R):
                    scale = 0.25 * time_step / (12.0 * (radius[i] + 0.5))
                    out[c, i, rows, lanes] = out[c, i, rows, lanes] - (weighted[i + 1] - weighted[i]) * scale

    channels = 3
    mine = pl.ds(channels * odd, channels)
    theirs = pl.ds(channels * (1 - odd), channels)

    def swap(k):
        return remote(own.at[k, theirs], got.at[k], c_send.at[k, 0], c_recv.at[k, 0], dict(theta=pair))

    def cross_over(k):
        return remote(half.at[k], cross.at[k], c_send.at[k, 1], c_recv.at[k, 1], dict(theta=across))

    def swap_back(k):
        return remote(
            whole_sum.at[k, mine], whole_sum.at[k, mine], c_send.at[k, 2], c_recv.at[k, 2], dict(theta=pair)
        )

    def stage_a(k):
        rows = slice(k * SUB, (k + 1) * SUB)
        block = jnp.concatenate([out[c, r, rows] for c in range(6) for r in range(nf)], 0)
        value = jnp.dot(block, table[...], preferred_element_type=jnp.float32, precision=lax.Precision.HIGHEST)
        own[k] = value.reshape(6, nf * SUB, value.shape[1])
        swap(k).start()

    def stage_b(k):
        swap(k).wait()
        half[k] = own[k, mine] + got[k]
        cross_over(k).start()

    def stage_c(k):
        cross_over(k).wait()
        whole_sum[k, mine] = half[k] + cross[k]
        swap_back(k).start()

    for k in range(chunks + 2):
        if k < chunks:

            @pl.when(first)
            def _():
                for copy in mirrored(k):
                    copy.wait()

            @pl.when(jnp.logical_not(first))
            def _():
                for copy in upward(k):
                    copy.wait_recv()

            @pl.when(jnp.logical_not(last))
            def _():
                for copy in downward(k):
                    copy.wait_recv()

            radial_chunk(k)

        @pl.when(first)
        def _():
            if k < chunks:
                stage_a(k)
            if 0 <= k - 1 < chunks:
                stage_b(k - 1)
            if 0 <= k - 2 < chunks:
                stage_c(k - 2)

    @pl.when(first)
    def _():
        for k in range(chunks):
            swap_back(k).wait()
            coef[k] = whole_sum[k]

    for k in range(chunks):

        @pl.when(jnp.logical_not(last))
        def _():
            for copy in upward_from(k):
                copy.wait_send()

        @pl.when(jnp.logical_not(first))
        def _():
            for copy in downward(k):
                copy.wait_send()


def inverse_kernel(nf, place, adv, coef, weights, table, out):
    _, R, Z, T = adv.shape
    first = place[0] == 1

    @pl.when(first)
    def _():
        for k in range(Z // SUB):
            rows = [
                coef[k, c, r * SUB : (r + 1) * SUB] * weights[r : r + 1] for c in range(6) for r in range(nf)
            ]
            value = lax.dot_general(
                jnp.concatenate(rows, 0),
                table[...],
                (((1,), (1,)), ((), ())),
                preferred_element_type=jnp.float32,
                precision=lax.Precision.HIGHEST,
            )
            for c in range(6):
                for r in range(nf):
                    at = (c * nf + r) * SUB
                    out[c, r, k * SUB : (k + 1) * SUB] = value[at : at + SUB]
        for c in range(6):
            for r in range(nf, R):
                out[c, r] = adv[c, r]

    @pl.when(jnp.logical_not(first))
    def _():
        out[...] = adv[...]


def build_table(positions, mode_count, length):
    orders = lax.iota(jnp.int32, mode_count)
    phases = positions[:, None] * orders[None, :] % length
    angles = phases.astype(jnp.float32) * (2.0 * math.pi / length)
    return jnp.concatenate([jnp.cos(angles), jnp.sin(angles)], 1)


def cycle_weights(cutoff, mode_count, length):
    orders = lax.iota(jnp.int32, mode_count)
    mode_scale = jnp.where(orders == 0, 1.0 / length, 2.0 / length)
    kept_modes = orders[None, :] <= cutoff[:, None]
    weight_half = jnp.where(kept_modes, mode_scale[None, :], 0.0)
    return jnp.concatenate([weight_half, weight_half], 1)


def shape_of(*dims):
    return jax.ShapeDtypeStruct(dims, jnp.float32)


def shards(state_start, state_section, phase, cutoff):
    row_count = lax.axis_size("row")
    row_id = lax.axis_index("row")
    theta_count = lax.axis_size("theta")
    theta_id = lax.axis_index("theta")
    gz_count = lax.axis_size("gz")
    _, R, Z, T = state_section.shape
    NL = R * Z
    nf = cutoff.shape[0]
    nl = T // LANES
    chunks = Z // SUB
    length = T * theta_count
    whole = pl.BlockSpec(memory_space=pltpu.VMEM)
    scalar = pl.BlockSpec(memory_space=pltpu.SMEM)

    radius = (row_id * R + lax.iota(jnp.int32, R + 1)).astype(jnp.float32)
    place = jnp.stack([row_id == 0, row_id == row_count - 1]).astype(jnp.int32)
    positions = theta_id * T + lax.iota(jnp.int32, T)
    table = build_table(positions, KMODES, length)
    weights = cycle_weights(cutoff, KMODES, length)
    ways = 2 * KMODES

    def vmem(*dims):
        return pltpu.VMEM(dims, jnp.float32)

    def dma(*dims):
        return pltpu.SemaphoreType.DMA(dims)

    advanced, coef = pl.pallas_call(
        functools.partial(fused_kernel, nf, 2.0 * math.pi / length, (row_count, theta_count, gz_count)),
        out_shape=[shape_of(6, R, Z, T), shape_of(chunks, 6, nf * SUB, ways)],
        in_specs=[scalar] + [whole] * 4,
        out_specs=[whole] * 2,
        scratch_shapes=[
            vmem(R, Z, T),
            vmem(7, R, nl, Z + 2 * SUB, LANES),
            pltpu.VMEM((R, nl, 2, SUB, LANES), jnp.int32),
            vmem(7, NL // LANES, T + 2 * SUB, LANES),
            vmem(6, NL // LANES, T, LANES),
            vmem(6, R, nl, Z, LANES),
            vmem(6, HALO, Z, T),
            pltpu.VMEM((HALO, Z, T), jnp.int32),
            vmem(6, HALO, Z, T),
            pltpu.VMEM((HALO, Z, T), jnp.int32),
            vmem(chunks, 6, nf * SUB, ways),
            vmem(chunks, 3, nf * SUB, ways),
            vmem(chunks, 3, nf * SUB, ways),
            vmem(chunks, 3, nf * SUB, ways),
            vmem(chunks, 6, nf * SUB, ways),
            dma(chunks, 2),
            dma(chunks, 2),
            dma(chunks, 2),
            dma(chunks, 2),
            dma(nl, 2, 2),
            dma(nl, 2, 2),
            dma(2),
            dma(2),
            dma(chunks, 5),
            dma(chunks, 3),
        ],
        compiler_params=pltpu.CompilerParams(
            vmem_limit_bytes=48 * 1024 * 1024, collective_id=0, has_side_effects=True
        ),
        name="fused",
    )(radius, state_start, state_section, phase, table)

    return pl.pallas_call(
        functools.partial(inverse_kernel, nf),
        out_shape=shape_of(6, R, Z, T),
        in_specs=[scalar] + [whole] * 4,
        out_specs=whole,
        compiler_params=pltpu.CompilerParams(vmem_limit_bytes=48 * 1024 * 1024),
        name="inverse",
    )(place, advanced, coef, weights, table)


def solution(mesh):
    in_specs = (
        P(None, "row", "gz", "theta"),
        P(None, "row", "gz", "theta"),
        P("row", "gz", "theta"),
        P(),
    )
    out_specs = P(None, "row", "gz", "theta")
    return jax.shard_map(shards, mesh=mesh, in_specs=in_specs, out_specs=out_specs, check_vma=False)
```

```python
import functools
import math

import jax
import jax.numpy as jnp
import numpy as np
from jax import lax
from jax.experimental import pallas as pl
from jax.experimental.pallas import tpu as pltpu
from jax.sharding import PartitionSpec as P

KMODES = 64
HALO = 3
LANES = 128
SUB = 8

split_speed = 10.0
time_step = 0.05
weno_epsilon = 1e-06
liquid_ratio = 4.4
gas_ratio = 1.4
liquid_stiffness = 0.6


def pressure_of(state, phase):
    kinetic = 0.5 * (state[1] * state[1] + state[2] * state[2] + state[3] * state[3]) / state[0]
    liquid = phase == 1
    heat_ratio = jnp.where(liquid, liquid_ratio, gas_ratio)
    stiffness = jnp.where(liquid, liquid_stiffness, 0.0)
    return (heat_ratio - 1.0) * (state[4] - kinetic) - heat_ratio * stiffness


def upwind_terms(f, count):
    D = [f[i + 1] - f[i] for i in range(count + 4)]
    G = [0.75 * D[i] for i in range(count + 4)]
    s = [D[i + 1] - D[i] for i in range(count + 3)]
    e = [s[i] - s[i + 1] for i in range(count + 2)]
    q = [s[i] * s[i] + 3.0 * weno_epsilon for i in range(count + 3)]
    out = []
    for m in range(count + 1):
        b0 = q[m] + G[m + 1] * (D[m + 1] + s[m])
        b1 = q[m + 1] + G[m + 1] * D[m + 2]
        b2 = q[m + 2] + G[m + 2] * (D[m + 2] - s[m + 2])
        B0 = b0 * (3.0 * b0)
        B1 = b1 * b1
        B2 = b2 * b2
        B2d = B2 + B2
        numer = B1 * (B2d * e[m] + B0 * e[m + 1])
        denom = B1 * (B2 + B0) + B0 * B2d
        r = pl.reciprocal(denom, approx=True)
        r = r * (2.0 - denom * r)
        out.append(numer * r)
    return out


def line_faces(q, velocity, pressure, component, channel, count):
    cells = count + 6
    flux = []
    for i in range(cells):
        if channel == 4:
            value = (q[i] + pressure(i)) * velocity[i]
        else:
            value = q[i] * velocity[i]
            if channel == component:
                value = value + pressure(i)
        flux.append(value)
    scaled = [split_speed * q[i] for i in range(cells)]
    plus = [flux[i] + scaled[i] for i in range(cells)]
    minus = [flux[i] - scaled[i] for i in range(cells)]
    up = upwind_terms(plus, count)
    down = upwind_terms(minus[::-1], count)[::-1]
    faces = []
    for m in range(count + 1):
        linear = 7.0 * (flux[m + 2] + flux[m + 3]) - (flux[m + 1] + flux[m + 4])
        linear = linear + ((scaled[m + 4] - scaled[m + 1]) - 3.0 * (scaled[m + 3] - scaled[m + 2]))
        faces.append(linear + (up[m] + down[m]))
    return faces


def fused_kernel(
    nf, length, counts, start_hbm, sec_hbm, phase_hbm, table_hbm, cutoff_hbm, out,
    table, start, sec, phase, cutoff, in_sem, press, fz, zph, fe, tt, zt, lo, loph, hi, hiph, own, got, half, cross, whole_sum,
    lo_send, lo_recv, hi_send, hi_recv, z_send, z_recv, t_send, t_recv, c_send, c_recv,
):
    row_count, theta_count, gz_count = counts
    _, R, Z, T = sec.shape
    NL = R * Z
    nl = T // LANES
    per = LANES // Z
    chunks = Z // SUB
    row = lax.axis_index("row")
    theta = lax.axis_index("theta")
    take_phase = pltpu.make_async_copy(phase_hbm, phase, in_sem.at[0])
    take_sec = pltpu.make_async_copy(sec_hbm, sec, in_sem.at[1])
    take_start = pltpu.make_async_copy(start_hbm, start, in_sem.at[2])
    take_table = pltpu.make_async_copy(table_hbm.at[pl.ds(theta * T, T)], table, in_sem.at[3])
    take_cutoff = pltpu.make_async_copy(cutoff_hbm, cutoff, in_sem.at[4])
    angle_step = 2.0 * math.pi / length
    take_sec.start()
    take_phase.start()
    radius = [(row * R + i).astype(jnp.float32) for i in range(R + 1)]
    gz = lax.axis_index("gz")
    first = row == 0
    last = row == row_count - 1
    MESH = pl.DeviceIdType.MESH

    right = lax.rem(theta + 1, theta_count)
    left = lax.rem(theta + theta_count - 1, theta_count)
    across = lax.rem(theta + theta_count // 2, theta_count)
    ahead = lax.rem(gz + 1, gz_count)
    behind = lax.rem(gz + gz_count - 1, gz_count)
    odd = lax.rem(theta, 2)
    pair = theta + 1 - 2 * odd

    barrier = pltpu.get_barrier_semaphore()

    def greet(**axes):
        pl.semaphore_signal(barrier, inc=1, device_id=axes, device_id_type=MESH)

    for t in (right, left, across):
        greet(theta=t)
    greet(gz=ahead)
    greet(gz=behind)

    @pl.when(jnp.logical_not(first))
    def _():
        greet(row=row - 1)

    @pl.when(jnp.logical_not(last))
    def _():
        greet(row=row + 1)

    @pl.when(jnp.logical_or(first, last))
    def _():
        pl.semaphore_wait(barrier, 6)

    if row_count > 2:

        @pl.when(jnp.logical_not(jnp.logical_or(first, last)))
        def _():
            pl.semaphore_wait(barrier, 7)

    def remote(src, dst, send, recv, axes):
        return pltpu.make_async_remote_copy(
            src_ref=src, dst_ref=dst, send_sem=send, recv_sem=recv, device_id=axes, device_id_type=MESH
        )

    def slab(k, g0, to, toph, send, recv, axes):
        zs = pl.ds(k * SUB, SUB)
        return (
            remote(sec.at[:, pl.ds(g0, HALO), zs], to.at[:, :, zs], send.at[k, 0], recv.at[k, 0], axes),
            remote(phase.at[pl.ds(g0, HALO), zs], toph.at[:, zs], send.at[k, 1], recv.at[k, 1], axes),
        )

    def mirrored(k):
        return slab(k, 0, lo, loph, lo_send, lo_recv, dict(theta=across))

    def upward(k):
        return slab(k, R - HALO, lo, loph, lo_send, lo_recv, dict(row=row + 1))

    def downward(k):
        return slab(k, 0, hi, hiph, hi_send, hi_recv, dict(row=row - 1))

    def start_all(copies):
        for copy in copies:
            copy.start()

    def mirror_start(k):
        @pl.when(first)
        def _():
            start_all(mirrored(k))

    take_sec.wait()
    take_phase.wait()
    mirror_start(0)

    def upward_from(k):
        zs = pl.ds(k * SUB, SUB)
        g0 = R - HALO
        axes = dict(row=row + 1)
        return (
            remote(sec.at[:, pl.ds(g0, HALO), zs], lo.at[:, :, zs], c_send.at[k, 3], lo_recv.at[k, 0], axes),
            remote(phase.at[pl.ds(g0, HALO), zs], loph.at[:, zs], c_send.at[k, 4], lo_recv.at[k, 1], axes),
        )

    for k in range(chunks):

        @pl.when(jnp.logical_not(last))
        def _():
            start_all(upward_from(k))

        @pl.when(jnp.logical_not(first))
        def _():
            start_all(downward(k))

    def axial_copies():
        out = []
        for n in range(nl):
            lanes = pl.ds(n * LANES, LANES)
            for side, (src0, dst0, axes) in enumerate(
                ((Z - SUB, 0, dict(gz=ahead)), (0, SUB + Z, dict(gz=behind)))
            ):
                rows = pl.ds(src0, SUB)
                out.append(
                    remote(
                        sec.at[:, :, rows, lanes],
                        fz.at[pl.ds(0, 6), :, n, pl.ds(dst0, SUB)],
                        z_send.at[n, side, 0],
                        z_recv.at[n, side, 0],
                        axes,
                    )
                )
                out.append(
                    remote(
                        phase.at[:, rows, lanes],
                        zph.at[:, n, side],
                        z_send.at[n, side, 1],
                        z_recv.at[n, side, 1],
                        axes,
                    )
                )
        return out

    start_all(axial_copies())
    take_start.start()
    take_table.start()
    take_cutoff.start()

    for r in range(R):
        press[r] = pressure_of([sec[c, r] for c in range(6)], phase[r])

    def field(c, r):
        return sec[c, r] if c < 6 else press[r]

    for c in range(7):
        for n in range(NL // LANES):
            block = jnp.concatenate([field(c, n * per + i) for i in range(per)], 0)
            fe[c, n, SUB : SUB + T] = jnp.transpose(block)
    for c in range(7):
        for r in range(R):
            value = field(c, r)
            for n in range(nl):
                fz[c, r, n, SUB : SUB + Z] = value[:, n * LANES : (n + 1) * LANES]

    def theta_copies():
        return (
            remote(
                fe.at[:, :, pl.ds(T, SUB)], fe.at[:, :, pl.ds(0, SUB)], t_send.at[0], t_recv.at[0], dict(theta=right)
            ),
            remote(
                fe.at[:, :, pl.ds(SUB, SUB)],
                fe.at[:, :, pl.ds(SUB + T, SUB)],
                t_send.at[1],
                t_recv.at[1],
                dict(theta=left),
            ),
        )

    start_all(theta_copies())
    for k in range(1, chunks):
        mirror_start(k)

    tstride = T // SUB
    chunk = SUB
    pieces = tstride // chunk

    def theta_piece(lane, k):
        base = k * chunk

        def at(c, i):
            return fe[c, lane, pl.ds(base + (i + SUB - HALO), SUB, stride=tstride), :]

        velocity = [at(2, i) / at(0, i) for i in range(chunk + 6)]
        for c in range(6):
            q = [at(c, i) for i in range(chunk + 6)]
            faces = line_faces(q, velocity, lambda i: at(6, i), 2, c, chunk)
            for m in range(chunk):
                tt[c, lane, pl.ds(base + m, SUB, stride=tstride), :] = faces[m + 1] - faces[m]

    for lane in range(NL // LANES):

        @pl.loop(1, pieces - 1)
        def _(k):
            theta_piece(lane, k)

    for copy in axial_copies():
        copy.wait()
    for side, row0 in enumerate((0, SUB + Z)):
        for r in range(R):
            for n in range(nl):
                cells = [fz[c, r, n, row0 : row0 + SUB] for c in range(6)]
                fz[6, r, n, row0 : row0 + SUB] = pressure_of(cells, zph[r, n, side])
    zstride = Z // SUB

    @pl.loop(0, R * nl)
    def _(step):
        r = step // nl
        n = step - r * nl

        def at(c, i):
            return fz[c, r, n, pl.ds(i + SUB - HALO, SUB, stride=zstride), :]

        velocity = [at(3, i) / at(0, i) for i in range(zstride + 6)]
        for c in range(6):
            q = [at(c, i) for i in range(zstride + 6)]
            faces = line_faces(q, velocity, lambda i: at(6, i), 3, c, zstride)
            for m in range(zstride):
                zt[c, r, n, pl.ds(m, SUB, stride=zstride), :] = faces[m + 1] - faces[m]

    for copy in theta_copies():
        copy.wait()
    for lane in range(NL // LANES):

        @pl.loop(0, 2)
        def _(k):
            theta_piece(lane, k * (pieces - 1))

    take_start.wait()
    for c in range(6):
        for n in range(NL // LANES):
            turned = jnp.transpose(tt[c, n])
            for i in range(per):
                r = n * per + i
                cell_radius = radius[r] + 0.5
                axial_part = jnp.concatenate([zt[c, r, m] for m in range(nl)], 1)
                tend = -(1.0 / 12.0) * axial_part - turned[i * Z : (i + 1) * Z] * (
                    1.0 / (12.0 * angle_step * cell_radius)
                )
                if c == 1:
                    tend = tend + (sec[2, r] * sec[2, r] / sec[0, r] + press[r]) / cell_radius
                if c == 2:
                    tend = tend - sec[1, r] * sec[2, r] / (sec[0, r] * cell_radius)
                out[c, r] = 0.75 * start[c, r] + 0.25 * (sec[c, r] + time_step * tend)

    take_table.wait()
    take_cutoff.wait()
    @pl.when(last)
    def _():
        for g in range(HALO):
            for c in range(6):
                hi[c, g] = sec[c, R - 1]
            hiph[g] = phase[R - 1]

    sign = jnp.where(first, -1.0, 1.0).astype(jnp.float32)

    def radial_chunk(k):
        rows = pl.ds(k * SUB, SUB)

        @pl.loop(0, nl)
        def _(n):
            lanes = pl.ds(pl.multiple_of(n * LANES, LANES), LANES)
            ghosts = {}
            for i in range(HALO):
                g = jnp.where(first, HALO - 1 - i, i)
                cells = [lo[c, g, rows, lanes] for c in range(6)]
                cells = [sign * v if c in (1, 2) else v for c, v in enumerate(cells)]
                ghosts[i] = cells + [pressure_of(cells, loph[g, rows, lanes])]
                cells = [hi[c, i, rows, lanes] for c in range(6)]
                ghosts[R + HALO + i] = cells + [pressure_of(cells, hiph[i, rows, lanes])]

            def at(c, i):
                if i in ghosts:
                    return ghosts[i][c]
                return sec[c, i - HALO, rows, lanes] if c < 6 else press[i - HALO, rows, lanes]

            velocity = [at(1, i) / at(0, i) for i in range(R + 6)]
            for c in range(6):
                q = [at(c, i) for i in range(R + 6)]
                faces = line_faces(q, velocity, lambda i: at(6, i), 1, c, R)
                weighted = [radius[i] * faces[i] for i in range(R + 1)]
                for i in range(R):
                    scale = 0.25 * time_step / (12.0 * (radius[i] + 0.5))
                    out[c, i, rows, lanes] = out[c, i, rows, lanes] - (weighted[i + 1] - weighted[i]) * scale

    channels = 3
    mine = pl.ds(channels * odd, channels)
    theirs = pl.ds(channels * (1 - odd), channels)

    def swap(k):
        return remote(own.at[k, theirs], got.at[k], c_send.at[k, 0], c_recv.at[k, 0], dict(theta=pair))

    def cross_over(k):
        return remote(half.at[k], cross.at[k], c_send.at[k, 1], c_recv.at[k, 1], dict(theta=across))

    def swap_back(k):
        return remote(
            whole_sum.at[k, mine], whole_sum.at[k, mine], c_send.at[k, 2], c_recv.at[k, 2], dict(theta=pair)
        )

    def stage_a(k):
        rows = slice(k * SUB, (k + 1) * SUB)
        block = jnp.concatenate([out[c, r, rows] for c in range(6) for r in range(nf)], 0)
        value = jnp.dot(block, table[...], preferred_element_type=jnp.float32, precision=lax.Precision.HIGHEST)
        own[k] = value.reshape(6, nf * SUB, value.shape[1])
        swap(k).start()

    def stage_b(k):
        swap(k).wait()
        half[k] = own[k, mine] + got[k]
        cross_over(k).start()

    def stage_c(k):
        cross_over(k).wait()
        whole_sum[k, mine] = half[k] + cross[k]
        swap_back(k).start()

    ways = table.shape[1]
    orders = lax.rem(lax.broadcasted_iota(jnp.int32, (SUB, ways), 1), ways // 2)
    mode_scale = jnp.where(orders == 0, 1.0 / length, 2.0 / length)

    def stage_d(k):
        swap_back(k).wait()
        kept = [jnp.where(orders <= cutoff[r], mode_scale, 0.0) for r in range(nf)]
        rows = [
            whole_sum[k, c, r * SUB : (r + 1) * SUB] * kept[r] for c in range(6) for r in range(nf)
        ]
        value = lax.dot_general(
            jnp.concatenate(rows, 0),
            table[...],
            (((1,), (1,)), ((), ())),
            preferred_element_type=jnp.float32,
            precision=lax.Precision.HIGHEST,
        )
        for c in range(6):
            for r in range(nf):
                at = (c * nf + r) * SUB
                out[c, r, k * SUB : (k + 1) * SUB] = value[at : at + SUB]

    for k in range(chunks + 3):
        if k < chunks:

            @pl.when(first)
            def _():
                for copy in mirrored(k):
                    copy.wait()

            @pl.when(jnp.logical_not(first))
            def _():
                for copy in upward(k):
                    copy.wait_recv()

            @pl.when(jnp.logical_not(last))
            def _():
                for copy in downward(k):
                    copy.wait_recv()

            radial_chunk(k)

        @pl.when(first)
        def _():
            if k < chunks:
                stage_a(k)
            if 0 <= k - 1 < chunks:
                stage_b(k - 1)
            if 0 <= k - 2 < chunks:
                stage_c(k - 2)
            if 0 <= k - 3:
                stage_d(k - 3)

    for k in range(chunks):

        @pl.when(jnp.logical_not(last))
        def _():
            for copy in upward_from(k):
                copy.wait_send()

        @pl.when(jnp.logical_not(first))
        def _():
            for copy in downward(k):
                copy.wait_send()


def full_table(mode_count, length):
    phases = np.outer(np.arange(length), np.arange(mode_count)) % length
    angles = phases * (2.0 * np.pi / length)
    return np.concatenate([np.cos(angles), np.sin(angles)], 1).astype(np.float32)


def shape_of(*dims):
    return jax.ShapeDtypeStruct(dims, jnp.float32)


def shards(state_start, state_section, phase, cutoff):
    row_count = lax.axis_size("row")
    theta_count = lax.axis_size("theta")
    gz_count = lax.axis_size("gz")
    _, R, Z, T = state_section.shape
    NL = R * Z
    nf = cutoff.shape[0]
    nl = T // LANES
    chunks = Z // SUB
    length = T * theta_count
    whole = pl.BlockSpec(memory_space=pltpu.VMEM)

    any_space = pl.BlockSpec(memory_space=pltpu.HBM)
    ways = 2 * KMODES

    def vmem(*dims):
        return pltpu.VMEM(dims, jnp.float32)

    def dma(*dims):
        return pltpu.SemaphoreType.DMA(dims)

    return pl.pallas_call(
        functools.partial(fused_kernel, nf, length, (row_count, theta_count, gz_count)),
        out_shape=shape_of(6, R, Z, T),
        in_specs=[any_space] * 5,
        out_specs=whole,
        scratch_shapes=[
            vmem(T, ways),
            vmem(6, R, Z, T),
            vmem(6, R, Z, T),
            pltpu.VMEM((R, Z, T), jnp.int32),
            pltpu.SMEM((nf,), jnp.int32),
            dma(5),
            vmem(R, Z, T),
            vmem(7, R, nl, Z + 2 * SUB, LANES),
            pltpu.VMEM((R, nl, 2, SUB, LANES), jnp.int32),
            vmem(7, NL // LANES, T + 2 * SUB, LANES),
            vmem(6, NL // LANES, T, LANES),
            vmem(6, R, nl, Z, LANES),
            vmem(6, HALO, Z, T),
            pltpu.VMEM((HALO, Z, T), jnp.int32),
            vmem(6, HALO, Z, T),
            pltpu.VMEM((HALO, Z, T), jnp.int32),
            vmem(chunks, 6, nf * SUB, ways),
            vmem(chunks, 3, nf * SUB, ways),
            vmem(chunks, 3, nf * SUB, ways),
            vmem(chunks, 3, nf * SUB, ways),
            vmem(chunks, 6, nf * SUB, ways),
            dma(chunks, 2),
            dma(chunks, 2),
            dma(chunks, 2),
            dma(chunks, 2),
            dma(nl, 2, 2),
            dma(nl, 2, 2),
            dma(2),
            dma(2),
            dma(chunks, 5),
            dma(chunks, 3),
        ],
        compiler_params=pltpu.CompilerParams(
            vmem_limit_bytes=65_500_000, collective_id=0, has_side_effects=True
        ),
        name="fused",
    )(state_start, state_section, phase, jnp.asarray(full_table(KMODES, length)), cutoff)


def solution(mesh):
    in_specs = (
        P(None, "row", "gz", "theta"),
        P(None, "row", "gz", "theta"),
        P("row", "gz", "theta"),
        P(),
    )
    out_specs = P(None, "row", "gz", "theta")
    return jax.shard_map(shards, mesh=mesh, in_specs=in_specs, out_specs=out_specs, check_vma=False)
```
